32 devices in a mesh: section: 2 (over core), expert: 16 (over z, y, x).
Axes of the slice: x: 2, y: 2, z: 4, core: 2. Of those that a mesh axis runs over, the one named last changes fastest.
Arguments:
- act_in: bfloat16 [2, 2048, 7168], P('section', 'expert'), may hold values from -6 to 6
- cotangent: bfloat16 [2, 2048, 7168], P('section', 'expert'), may hold values from -6 to 6
- fwd_ids: int32 [2, 2048, 8], P('section', 'expert'), may hold values from 0 to 255, as said below
- fwd_gates: float32 [2, 2048, 8], P('section', 'expert'), may hold values from 0.05 to 0.8
- bwd_ids: int32 [2, 2048, 8], P('section', 'expert'), may hold values from 0 to 255, as said below
- bwd_gates: float32 [2, 2048, 8], P('section', 'expert'), may hold values from 0.05 to 0.8
- gate_w: bfloat16 [2, 7168, 2048], P('section', None, 'expert'), may hold values from -0.0625 to 0.0625
- up_w: bfloat16 [2, 7168, 2048], P('section', None, 'expert'), may hold values from -0.0625 to 0.0625
- down_w: bfloat16 [2, 2048, 7168], P('section', 'expert'), may hold values from -0.125 to 0.125
- gate_pre: bfloat16 [2, 160, 2048], P('section', None, 'expert'), may hold values from -6 to 6
- up_pre: bfloat16 [2, 160, 2048], P('section', None, 'expert'), may hold values from -6 to 6
Outputs:
- next_act: bfloat16 [2, 2048, 7168], P('section', 'expert')
- prev_grad: bfloat16 [2, 2048, 7168], P('section', 'expert')
- gate_grad: float32 [2, 2048, 8], P('section', 'expert')
The draws below stay inside these ranges and needn't reach their ends.
Inputs may be any that keep to these rules, and one draw needn't show every extreme that they name: `fwd_ids`: the 8 ids of a row differ. In each aligned block of 128 rows (the rows of one device) each id below 1 is named by at most 10 rows; in every section one such id is named by exactly 10 rows in every block. `bwd_ids`: as for fwd_ids.
All inputs are finite; a program needn't handle non-finite values.
Results may differ from the reference program's by a relative error of at most 0.012.
Values may be sent and summed in bfloat16 or wider, within the bound.
A program may use at most 128 MiB of HBM per device.

```python
import math
import jax
import jax.numpy as jnp
from jax import lax

D = 7168
FF = 2048
ROUTED = 256
TOP = 8
TOK_DEV = 128
CAP = 10
SLICES = 16
FF_DEV = 128
EXPERTS = 1
SECTIONS = 2
TOKENS = 2048
SLOTS = 160


def route_draw(key):
    blocks = SECTIONS * (TOKENS // TOK_DEV)
    keys = [jax.random.fold_in(key, offset) for offset in range(5)]
    counts = jax.random.randint(keys[0], (blocks, EXPERTS), CAP // 2, CAP + 1)
    fullest = jax.random.randint(keys[1], (SECTIONS,), 0, EXPERTS)
    fullest_block = jnp.repeat(fullest, TOKENS // TOK_DEV)
    counts = jnp.where(jnp.arange(EXPERTS)[None, :] == fullest_block[:, None], CAP, counts)
    scores = jax.random.randint(keys[2], (blocks, EXPERTS, TOK_DEV), 0, 2 ** 20) * TOK_DEV + jnp.arange(TOK_DEV)
    order = jnp.argsort(jnp.argsort(scores, axis=-1), axis=-1)
    chosen = order < counts[:, :, None]
    others = jax.random.randint(keys[3], (blocks, TOK_DEV, ROUTED - EXPERTS), 0, 2 ** 20) * ROUTED + jnp.arange(ROUTED - EXPERTS)
    unused, picks = lax.top_k(others, TOP)
    ids = picks + EXPERTS
    slot_scores = jax.random.randint(keys[4], (blocks, TOK_DEV, TOP), 0, 2 ** 20) * TOP + jnp.arange(TOP)
    unused_two, places = lax.top_k(slot_scores, TOP)
    slot_iota = jnp.arange(TOP)
    for expert in range(EXPERTS):
        target = places[:, :, expert:expert + 1]
        put_here = (slot_iota[None, None, :] == target) & chosen[:, expert, :, None]
        ids = jnp.where(put_here, expert, ids)
    return ids.reshape(SECTIONS, TOKENS, TOP).astype(jnp.int32)


def draw_fwd_ids(key, part):
    return route_draw(jax.random.fold_in(key, 11))


def draw_bwd_ids(key, part):
    return route_draw(jax.random.fold_in(key, 23))


def block_scale(key, extent, pieces, least, high):
    def one(dim, shards_of):
        draws = jax.random.uniform(jax.random.fold_in(jax.random.fold_in(key, 6), dim), (shards_of,), jnp.float32, least / len(pieces), high / len(pieces))
        return jnp.repeat(jnp.exp(draws), extent[dim] // shards_of).reshape((-1,) + (1,) * (len(extent) - dim - 1))

    level = one(*pieces[0])
    for cut in pieces[1:]:
        level = level * one(*cut)
    return level


def scatter_about(key, shape, width, reach, shards=(), held_as=jnp.bfloat16):
    values = width * jax.random.normal(key, shape, jnp.float32)
    if shards:
        values = values * block_scale(key, shape, shards, -0.22, 0.18)
    return jnp.clip(values, -reach, reach).astype(held_as)


def setup_inputs(seed: int = 0) -> dict:
    streams_of = jax.random.split(jax.random.key(seed), 12)
    return {
        "act_in": scatter_about(streams_of[0], (SECTIONS, TOKENS, D), 1.0, 6.0, ((0, 2), (1, 16))),
        "cotangent": scatter_about(streams_of[1], (SECTIONS, TOKENS, D), 1.0, 6.0, ((0, 2), (1, 16))),
        "fwd_ids": draw_fwd_ids(jax.random.fold_in(streams_of[11], 71), 0),
        "fwd_gates": jnp.clip(jnp.exp(math.log(0.8) - 2.7725887 * jax.random.uniform(streams_of[3], (SECTIONS, TOKENS, TOP), jnp.float32) ** block_scale(streams_of[3], (SECTIONS, TOKENS, TOP), ((0, 2), (1, 16)), -0.2, 0.2)), 0.05, 0.8),
        "bwd_ids": draw_bwd_ids(jax.random.fold_in(streams_of[11], 71), 0),
        "bwd_gates": jnp.clip(jnp.exp(math.log(0.8) - 2.7725887 * jax.random.uniform(streams_of[5], (SECTIONS, TOKENS, TOP), jnp.float32) ** block_scale(streams_of[5], (SECTIONS, TOKENS, TOP), ((0, 2), (1, 16)), -0.2, 0.2)), 0.05, 0.8),
        "gate_w": scatter_about(streams_of[6], (SECTIONS, D, EXPERTS * FF), D ** -0.5, 0.0625, ((0, 2), (2, 16))),
        "up_w": scatter_about(streams_of[7], (SECTIONS, D, EXPERTS * FF), D ** -0.5, 0.0625, ((0, 2), (2, 16))),
        "down_w": scatter_about(streams_of[8], (SECTIONS, EXPERTS * FF, D), FF ** -0.5, 0.125, ((0, 2), (1, 16))),
        "gate_pre": scatter_about(streams_of[9], (SECTIONS, SLOTS, EXPERTS * FF), 1.0, 6.0, ((0, 2), (2, 16))),
        "up_pre": scatter_about(streams_of[10], (SECTIONS, SLOTS, EXPERTS * FF), 1.0, 6.0, ((0, 2), (2, 16))),
    }


def slots_of(ids, expert):
    matches = ids == expert
    routed = jnp.any(matches, axis=1)
    blocks = routed.reshape(-1, TOK_DEV).astype(jnp.int32)
    position = (jnp.cumsum(blocks, axis=1) - 1).reshape(-1)
    block_ids = jnp.arange(TOKENS, dtype=jnp.int32) // TOK_DEV
    slot = jnp.where(routed, block_ids * CAP + position, SLOTS).astype(jnp.int32)
    return matches, slot


def place_rows(tokens, slot):
    empty = jnp.zeros((SLOTS, tokens.shape[1]), tokens.dtype)
    return empty.at[slot].set(tokens, mode="drop")


def take_rows(table, slot):
    return jnp.take(table, jnp.minimum(slot, SLOTS - 1).astype(jnp.int32), axis=0)


def rounded_sum(parts):
    rounded = lax.optimization_barrier(parts.astype(jnp.bfloat16))
    return jnp.sum(rounded.astype(jnp.float32), axis=0)


def section_layer(tokens, grads, ids_f, gates_f, ids_b, gates_b, w_gate, w_up, w_down, pre_gate, pre_up):
    mixed = jnp.zeros((TOKENS, D), jnp.float32)
    input_grad = jnp.zeros((TOKENS, D), jnp.float32)
    gate_grad = jnp.zeros((TOKENS, TOP), jnp.float32)
    for expert in range(EXPERTS):
        lo_col = expert * FF
        wg_e = w_gate[:, lo_col:lo_col + FF]
        wu_e = w_up[:, lo_col:lo_col + FF]
        wd_e = w_down[lo_col:lo_col + FF]
        matches, slot = slots_of(ids_f, expert)
        weights = jnp.sum(jnp.where(matches, gates_f, 0.0), axis=1)
        rows = place_rows(tokens, slot)
        gate_act = jnp.dot(rows, wg_e, preferred_element_type=jnp.float32)
        up_act = jnp.dot(rows, wu_e, preferred_element_type=jnp.float32)
        hidden = (jax.nn.silu(gate_act) * up_act).astype(jnp.bfloat16)
        parts = jnp.einsum("rsf,sfd->srd", hidden.reshape(SLOTS, SLICES, FF_DEV).astype(jnp.float32),
                           wd_e.reshape(SLICES, FF_DEV, D).astype(jnp.float32))
        expert_out = rounded_sum(parts)
        mixed = mixed + weights[:, None] * take_rows(expert_out, slot)

        matches_b, slot_b = slots_of(ids_b, expert)
        weights_b = jnp.sum(jnp.where(matches_b, gates_b, 0.0), axis=1)
        grad_rows = place_rows(grads, slot_b)
        saved_gate = pre_gate[:, lo_col:lo_col + FF].astype(jnp.float32)
        saved_up = pre_up[:, lo_col:lo_col + FF].astype(jnp.float32)
        grad_hidden = jnp.dot(grad_rows, wd_e.T, preferred_element_type=jnp.float32)
        sigmoid_gate = jax.nn.sigmoid(saved_gate)
        activated = saved_gate * sigmoid_gate
        dot_parts = jnp.sum((grad_hidden * activated * saved_up).reshape(SLOTS, SLICES, FF_DEV), axis=2)
        expert_dot = rounded_sum(dot_parts.T)
        grad_gate_act = (grad_hidden * saved_up * sigmoid_gate * (1.0 + saved_gate * (1.0 - sigmoid_gate))).astype(jnp.bfloat16)
        grad_up_act = (grad_hidden * activated).astype(jnp.bfloat16)
        grad_parts = jnp.einsum("rsf,dsf->srd", grad_gate_act.reshape(SLOTS, SLICES, FF_DEV).astype(jnp.float32),
                                wg_e.reshape(D, SLICES, FF_DEV).astype(jnp.float32))
        grad_parts = grad_parts + jnp.einsum("rsf,dsf->srd", grad_up_act.reshape(SLOTS, SLICES, FF_DEV).astype(jnp.float32),
                                             wu_e.reshape(D, SLICES, FF_DEV).astype(jnp.float32))
        expert_grad = rounded_sum(grad_parts)
        input_grad = input_grad + weights_b[:, None] * take_rows(expert_grad, slot_b)
        gate_grad = gate_grad + jnp.where(matches_b, take_rows(expert_dot, slot_b)[:, None], 0.0)
    return mixed.astype(jnp.bfloat16), input_grad.astype(jnp.bfloat16), gate_grad


def reference(act_in, cotangent, fwd_ids, fwd_gates, bwd_ids, bwd_gates, gate_w, up_w, down_w, gate_pre, up_pre):
    outputs = []
    grads = []
    gate_grads = []
    for section in range(SECTIONS):
        mixed, input_grad, gate_grad = section_layer(act_in[section], cotangent[section], fwd_ids[section], fwd_gates[section],
                                                   bwd_ids[section], bwd_gates[section], gate_w[section], up_w[section],
                                                   down_w[section], gate_pre[section], up_pre[section])
        outputs.append(mixed)
        grads.append(input_grad)
        gate_grads.append(gate_grad)
    next_act = jnp.roll(jnp.stack(outputs), 1, axis=0)
    prev_grad = jnp.roll(jnp.stack(grads), -1, axis=0)
    return next_act, prev_grad, jnp.stack(gate_grads)
```

```python
import functools
import math

import jax
import jax.numpy as jnp
from jax import lax
from jax.experimental import pallas as pl
from jax.experimental.pallas import tpu as pltpu
from jax.sharding import PartitionSpec as P

FF = 2048
QUAD = 4
MESH = pl.DeviceIdType.MESH


def from_behind(value, axis, steps):
    count = lax.axis_size(axis)
    pairs = [(source, (source + steps) % count) for source in range(count)]
    return lax.ppermute(value, axis, pairs)


def routing(ids, gates, experts, capacity):
    expert_ids = jnp.arange(experts, dtype=jnp.int32)
    matches = ids[None, :, :] == expert_ids[:, None, None]
    routed = jnp.any(matches, axis=2)
    weights = jnp.sum(jnp.where(matches, gates[None, :, :], 0.0), axis=2)
    tokens = ids.shape[0]
    earlier = jnp.arange(tokens)[:, None] <= jnp.arange(tokens)[None, :]
    counted = jnp.sum(jnp.where(routed[:, :, None] & earlier[None], 1, 0), axis=1)
    position = counted - 1
    slot_ids = jnp.arange(capacity, dtype=jnp.int32)
    placing = (position[:, None, :] == slot_ids[None, :, None]) & routed[:, None, :]
    return (matches, placing.astype(jnp.float32), weights)


def xor(value, mask):
    out = value
    bit = 1
    while bit <= mask:
        if mask & bit:
            out = out + bit - 2 * bit * ((value // bit) % 2)
        bit *= 2
    return out


def dot(a, b, dims=((1,), (0,)), precision=None):
    return lax.dot_general(
        a, b, (dims, ((), ())), preferred_element_type=jnp.float32, precision=precision
    )


class Links:
    def __init__(self, send_sems, recv_sems):
        self.send_sems = send_sems
        self.recv_sems = recv_sems
        self.count = 0
        self.sent = []

    def copy(self, src, dst, peer):
        k = self.count
        self.count += 1
        return pltpu.make_async_remote_copy(
            src_ref=src,
            dst_ref=dst,
            send_sem=self.send_sems.at[k],
            recv_sem=self.recv_sems.at[k],
            device_id={"expert": peer},
            device_id_type=MESH,
        )

    def start(self, copy):
        copy.start()
        self.sent.append(copy)


def layer_kernel(
    slices,
    chunks,
    tok_f,
    tok_b,
    w_gate,
    w_up,
    w_down,
    place_f,
    place_b,
    pre_gate,
    pre_up,
    rid_ref,
    fold_ref,
    unfold_ref,
    spread_ref,
    collect_ref,
    out_f,
    out_b,
    out_dots,
    tok,
    wc,
    wd,
    gat,
    par,
    rs1,
    rs2,
    rsz,
    hold,
    hold2,
    acc_ref,
    dot_ref,
    dot_got,
    local_sems,
    send_sems,
    recv_sems,
):
    device = lax.axis_index("expert")
    me = device % slices
    base = device - me
    lo = me % QUAD
    z = me // QUAD
    depth = slices // QUAD
    xp = base + xor(me, 1)
    yp = base + xor(me, 2)
    zp = [base + xor(z, q) * QUAD + lo for q in range(depth)]
    partners = [xp, yp] + zp[1:]
    width = wd.shape[2]
    ff = wd.shape[1]

    loads = []

    def load(src, dst):
        copy = pltpu.make_async_copy(src, dst, local_sems.at[len(loads)])
        loads.append(copy)
        copy.start()
        return copy

    load_tok = [load(tok_f, tok.at[0]), load(tok_b, tok.at[1])]
    load_w = []
    for j in range(chunks):
        rows = pl.ds(j * width, width)
        load_w.append(load(w_gate.at[rows, :], wc.at[j, :, pl.ds(0, ff)]))
        load_w.append(load(w_up.at[rows, :], wc.at[j, :, pl.ds(ff, ff)]))
        load_w.append(load(w_down.at[:, rows], wd.at[j]))

    barrier = pltpu.get_barrier_semaphore()
    for peer in partners:
        pl.semaphore_signal(barrier, inc=1, device_id={"expert": peer}, device_id_type=MESH)

    block_rows = gat.shape[2]
    group_rows = QUAD * block_rows
    places = (place_f, place_b)

    def place(mb):
        rid = rid_ref[:block_rows, :1]
        chosen = places[mb][...]
        total = jnp.zeros((block_rows, width), jnp.float32)
        for j in range(chunks):
            part = jnp.where(rid == j, chosen, 0.0).astype(jnp.bfloat16)
            total = total + dot(part, tok[mb, :, pl.ds(j * width, width)])
        gat[mb, me] = total.astype(jnp.bfloat16)

    links = Links(send_sems, recv_sems)

    def bid(q, mask):
        return xor(z, q) * QUAD + xor(lo, mask)

    steps = [(mb, q) for mb in range(2) for q in range(depth)]
    zsend = {}
    own_x, own_y, forward = {}, {}, {}
    r1, r2, rz = {}, {}, {}
    for mb, q in steps:
        if q > 0:
            zsend[mb, q] = links.copy(gat.at[mb, me], gat.at[mb, me], zp[q])
        block = gat.at[mb, bid(q, 0)]
        own_x[mb, q] = links.copy(block, block, xp)
        own_y[mb, q] = links.copy(block, block, yp)
        first = q % 2 == 0
        got = gat.at[mb, bid(q, 2 if first else 1)]
        forward[mb, q] = links.copy(got, got, xp if first else yp)
        m1, p1, m2, p2 = (1, xp, 2, yp) if first else (2, yp, 1, xp)
        r1[mb, q] = [
            links.copy(par.at[mb, bid(q, m1)], rs1.at[mb, q, 0], p1),
            links.copy(par.at[mb, bid(q, 3)], rs1.at[mb, q, 1], p1),
        ]
        r2[mb, q] = links.copy(hold.at[mb, q], rs2.at[mb, q], p2)
        if q > 0:
            rz[mb, q] = links.copy(hold2.at[mb, q], rsz.at[mb, q], zp[q])
    dx = links.copy(dot_ref.at[0], dot_got.at[0], xp)
    dy = links.copy(dot_ref.at[1], dot_got.at[1], yp)
    dz = [links.copy(dot_ref.at[2], dot_got.at[1 + q], zp[q]) for q in range(1, depth)]

    def own_sends(mb, q):
        if q > 0:
            zsend[mb, q].wait_recv()
        links.start(own_x[mb, q])
        links.start(own_y[mb, q])

    def start_mb(mb):
        for q in range(1, depth):
            links.start(zsend[mb, q])

    def do_forward(mb, q):
        (own_y if q % 2 == 0 else own_x)[mb, q].wait_recv()
        links.start(forward[mb, q])

    def compute(mb, q):
        (own_x if q % 2 == 0 else own_y)[mb, q].wait_recv()
        forward[mb, q].wait_recv()
        zq = xor(z, q)
        rid = rid_ref[...]
        group = pl.ds(zq * QUAD, QUAD)
        buf = gat[mb, group].reshape(group_rows, width)
        half = rid[:, :ff]
        fold = fold_ref[...]
        unfold = unfold_ref[...]
        if mb == 0:

            def gather_step(j, acc):
                return jnp.where(rid == j.astype(jnp.float32), dot(buf, wc[j]), acc)

            acc = lax.fori_loop(0, chunks, gather_step, jnp.zeros((group_rows, 2 * ff), jnp.float32))
            act = dot(fold, acc, precision=lax.Precision.HIGHEST)
            gate = act[:, :ff]
            hidden = gate / (1.0 + jnp.exp(-gate)) * act[:, ff:]
            spread = dot(unfold, hidden.astype(jnp.bfloat16))
            acc_ref[...] = jnp.zeros_like(acc_ref)

            def out_step(j, carry):
                part = jnp.where(half == j.astype(jnp.float32), spread, 0.0).astype(jnp.bfloat16)
                acc_ref[...] += dot(part, wd[j])
                return carry

            lax.fori_loop(0, chunks, out_step, 0)
        else:

            def gather_step(j, acc):
                return jnp.where(
                    half == j.astype(jnp.float32), dot(buf, wd[j], ((1,), (1,))), acc
                )

            acc = lax.fori_loop(0, chunks, gather_step, jnp.zeros((group_rows, ff), jnp.float32))
            grad = dot(fold, acc, precision=lax.Precision.HIGHEST)
            count = grad.shape[0]
            gate = pre_gate[zq].astype(jnp.float32)
            up = pre_up[zq].astype(jnp.float32)
            sig = 1.0 / (1.0 + jnp.exp(-gate))
            activated = gate * sig
            dots = jnp.sum(grad * activated * up, axis=1, keepdims=True)
            tile = dot(
                collect_ref[...], dots * spread_ref[...], precision=lax.Precision.HIGHEST
            )
            dot_ref[0, zq] = tile
            grad_gate = (grad * up * sig * (1.0 + gate * (1.0 - sig))).astype(jnp.bfloat16)
            grad_up = (grad * activated).astype(jnp.bfloat16)
            spread = jnp.concatenate([dot(unfold, grad_gate), dot(unfold, grad_up)], axis=1)
            acc_ref[...] = jnp.zeros_like(acc_ref)

            def out_step(j, carry):
                part = jnp.where(rid == j.astype(jnp.float32), spread, 0.0).astype(jnp.bfloat16)
                acc_ref[...] += dot(part, wc[j], ((1,), (1,)))
                return carry

            lax.fori_loop(0, chunks, out_step, 0)
        par[mb, group] = acc_ref[...].astype(jnp.bfloat16).reshape(QUAD, block_rows, width)
        for copy in r1[mb, q]:
            links.start(copy)

    def wide(value):
        return value.astype(jnp.float32)

    def second(mb, q):
        for copy in r1[mb, q]:
            copy.wait_recv()
        m2 = 2 if q % 2 == 0 else 1
        total = wide(par[mb, bid(q, m2)]) + wide(rs1[mb, q, 1])
        hold[mb, q] = total.astype(jnp.bfloat16)
        links.start(r2[mb, q])

    def third(mb, q):
        r2[mb, q].wait_recv()
        total = wide(par[mb, bid(q, 0)]) + wide(rs1[mb, q, 0]) + wide(rs2[mb, q])
        hold2[mb, q] = total.astype(jnp.bfloat16)
        if q > 0:
            links.start(rz[mb, q])

    def finish(mb, out):
        total = wide(hold2[mb, 0])
        for q in range(1, depth):
            rz[mb, q].wait_recv()
            total = total + wide(rsz[mb, q])
        out[...] = total.astype(jnp.bfloat16)

    load_tok[0].wait()
    place(0)
    pl.semaphore_wait(barrier, len(partners))
    start_mb(0)
    own_sends(*steps[0])
    load_tok[1].wait()
    place(1)
    for copy in load_w:
        copy.wait()
    count = len(steps)
    for t in range(count + 3):
        if t + 1 < count:
            if t + 1 == 2:
                start_mb(1)
            own_sends(*steps[t + 1])
        if t < count:
            do_forward(*steps[t])
        if 0 <= t - 1 < count:
            compute(*steps[t - 1])
        if t - 1 == count - 1:
            links.start(dx)
        if 0 <= t - 2 < count:
            second(*steps[t - 2])
        if t - 2 == count - 1:
            dx.wait_recv()
            dot_ref[1] = dot_ref[0] + dot_got[0]
            links.start(dy)
        if 0 <= t - 3 < count:
            third(*steps[t - 3])
    finish(0, out_f)
    dy.wait_recv()
    dot_ref[2] = dot_ref[1] + dot_got[1]
    for copy in dz:
        links.start(copy)
    finish(1, out_b)
    total = dot_ref[2]
    for q in range(1, depth):
        dz[q - 1].wait_recv()
        total = total + dot_got[1 + q]
    out_dots[...] = total
    for copy in links.sent:
        copy.wait_send()


def run_layer(tok_f, tok_b, w_gate, w_up, w_down, place_f, place_b, pre_gate, pre_up, slices, rows):
    features = tok_f.shape[1]
    chunks = 16 // math.gcd(16, rows)
    width = features // chunks
    ff = w_gate.shape[1]
    depth = slices // QUAD
    block_rows = chunks * rows
    group_rows = QUAD * block_rows
    group_slots = QUAD * rows

    row = jnp.arange(group_rows)
    slot = (row // block_rows) * rows + row % rows
    rid = jnp.broadcast_to((row % block_rows // rows)[:, None], (group_rows, 2 * ff))
    rid = rid.astype(jnp.float32)
    unfold = (slot[:, None] == jnp.arange(group_slots)[None, :])
    fold = unfold.T.astype(jnp.float32)
    unfold = unfold.astype(jnp.bfloat16)
    slots = jnp.arange(group_slots)
    spread = (slots[:, None] % rows == jnp.arange(128)[None, :]).astype(jnp.float32)
    collect = (slots[None, :] // rows == jnp.arange(8)[:, None]).astype(jnp.float32)

    vmem = pl.BlockSpec(memory_space=pltpu.VMEM)
    anywhere = pl.BlockSpec(memory_space=pl.ANY)
    block = (block_rows, width)
    sems = 2 * (depth * 6 + 2 * (depth - 1)) + 2 + depth - 1
    return pl.pallas_call(
        functools.partial(layer_kernel, slices, chunks),
        out_shape=(
            jax.ShapeDtypeStruct(block, jnp.bfloat16),
            jax.ShapeDtypeStruct(block, jnp.bfloat16),
            jax.ShapeDtypeStruct((depth, 8, 128), jnp.float32),
        ),
        in_specs=[anywhere] * 5 + [vmem] * 9,
        out_specs=(vmem, vmem, vmem),
        scratch_shapes=[
            pltpu.VMEM((2,) + tok_f.shape, jnp.bfloat16),
            pltpu.VMEM((chunks, width, 2 * ff), jnp.bfloat16),
            pltpu.VMEM((chunks, ff, width), jnp.bfloat16),
            pltpu.VMEM((2, slices) + block, jnp.bfloat16),
            pltpu.VMEM((2, slices) + block, jnp.bfloat16),
            pltpu.VMEM((2, depth, 2) + block, jnp.bfloat16),
            pltpu.VMEM((2, depth) + block, jnp.bfloat16),
            pltpu.VMEM((2, depth) + block, jnp.bfloat16),
            pltpu.VMEM((2, depth) + block, jnp.bfloat16),
            pltpu.VMEM((2, depth) + block, jnp.bfloat16),
            pltpu.VMEM((group_rows, width), jnp.float32),
            pltpu.VMEM((3, depth, 8, 128), jnp.float32),
            pltpu.VMEM((1 + depth, depth, 8, 128), jnp.float32),
            pltpu.SemaphoreType.DMA((2 + 3 * chunks,)),
            pltpu.SemaphoreType.DMA((sems,)),
            pltpu.SemaphoreType.DMA((sems,)),
        ],
        compiler_params=pltpu.CompilerParams(
            collective_id=0, has_side_effects=True, vmem_limit_bytes=56 * 2**20
        ),
        name="moe_layer",
    )(tok_f, tok_b, w_gate, w_up, w_down, place_f, place_b, pre_gate, pre_up,
      rid, fold, unfold, spread, collect)


def mix_kernel(rows, block_f, block_b, weight_f, weight_b, out_f, out_b):
    block_rows, width = block_f.shape
    j = pl.program_id(0)
    low = j * rows
    column = lax.broadcasted_iota(jnp.int32, weight_f.shape, 1)
    inside = (column >= low) & (column < low + rows)
    for block, weight, out in ((block_f, weight_f, out_f), (block_b, weight_b, out_b)):
        wanted = jnp.where(inside, weight[...], 0.0)
        high = wanted.astype(jnp.bfloat16)
        rest = (wanted - high.astype(jnp.float32)).astype(jnp.bfloat16)
        out[...] = (dot(high, block[...]) + dot(rest, block[...])).astype(jnp.bfloat16)


def mix(block_f, block_b, weight_f, weight_b, rows):
    block_rows, width = block_f.shape
    tokens = weight_f.shape[0]
    chunks = block_rows // rows
    whole = pl.BlockSpec(block_f.shape, lambda j: (0, 0))
    weights = pl.BlockSpec(weight_f.shape, lambda j: (0, 0))
    piece = pl.BlockSpec((tokens, width), lambda j: (0, j))
    shape = jax.ShapeDtypeStruct((tokens, chunks * width), jnp.bfloat16)
    return pl.pallas_call(
        functools.partial(mix_kernel, rows),
        out_shape=(shape, shape),
        grid=(chunks,),
        in_specs=[whole, whole, weights, weights],
        out_specs=(piece, piece),
        name="mix",
    )(block_f, block_b, weight_f, weight_b)


def body(
    act_in,
    cotangent,
    fwd_ids,
    fwd_gates,
    bwd_ids,
    bwd_gates,
    gate_w,
    up_w,
    down_w,
    gate_pre,
    up_pre,
):
    ndev = lax.axis_size("expert")
    ff_dev = gate_w.shape[2]
    slices = FF // ff_dev
    experts = ndev // slices
    capacity = gate_pre.shape[1] // ndev
    rows = experts * capacity
    chunks = 16 // math.gcd(16, rows)
    features = act_in.shape[2]
    width = features // chunks
    depth = slices // QUAD
    columns = [[g * slices + i for g in range(experts)] for i in range(slices)]

    def exchange(value):
        return lax.all_to_all(
            value, "expert", split_axis=0, concat_axis=0, axis_index_groups=columns, tiled=True
        )

    matches_f, placing_f, weights_f = routing(fwd_ids[0], fwd_gates[0], experts, capacity)
    matches_b, placing_b, weights_b = routing(bwd_ids[0], bwd_gates[0], experts, capacity)

    def prepare(tokens, placing):
        chosen = placing.reshape(rows, tokens.shape[0])
        if experts > 1:
            picked = dot(chosen.astype(jnp.bfloat16), tokens).astype(jnp.bfloat16)
            picked = exchange(picked.reshape(experts, capacity, features))
            tokens = picked.reshape(rows, features)
            chosen = jnp.eye(rows, dtype=jnp.float32)
        return tokens, jnp.tile(chosen, (chunks, 1))

    tok_f, place_f = prepare(act_in[0], placing_f)
    tok_b, place_b = prepare(cotangent[0], placing_b)

    def by_group(saved):
        saved = saved.reshape(experts, slices, capacity, ff_dev).transpose(1, 0, 2, 3)
        return saved.reshape(depth, QUAD * rows, ff_dev)

    block_f, block_b, dots = run_layer(
        tok_f, tok_b, gate_w[0], up_w[0], down_w[0], place_f, place_b,
        by_group(gate_pre[0]), by_group(up_pre[0]), slices, rows,
    )
    me = lax.axis_index("expert") % slices
    mine = lax.dynamic_slice(dots, (me // QUAD, me % QUAD, 0), (1, 1, 128))
    mine = mine[0, 0, :rows].reshape(experts, capacity)

    def send_back(block):
        table = block.reshape(chunks, rows, width).transpose(1, 0, 2)
        table = exchange(table.reshape(experts, capacity, features))
        table = table.reshape(rows, chunks, width).transpose(1, 0, 2)
        return table.reshape(chunks * rows, width)

    if experts > 1:
        block_f = send_back(block_f)
        block_b = send_back(block_b)
        mine = exchange(mine)

    token_dots = jnp.sum(placing_b * mine[:, :, None], axis=1)
    gate_grad = jnp.sum(jnp.where(matches_b, token_dots[:, :, None], 0.0), axis=0)

    def weight_table(placing, weights):
        table = (placing * weights[:, None, :]).reshape(rows, -1).T
        return jnp.tile(table, (1, chunks))

    weight_f = from_behind(weight_table(placing_f, weights_f), "section", 1)
    weight_b = from_behind(weight_table(placing_b, weights_b), "section", -1)
    block_f = from_behind(block_f, "section", 1)
    block_b = from_behind(block_b, "section", -1)
    next_act, prev_grad = mix(block_f, block_b, weight_f, weight_b, rows)
    return (next_act[None], prev_grad[None], gate_grad[None])


def solution(mesh):
    in_specs = (
        P("section", "expert", None),
        P("section", "expert", None),
        P("section", "expert", None),
        P("section", "expert", None),
        P("section", "expert", None),
        P("section", "expert", None),
        P("section", None, "expert"),
        P("section", None, "expert"),
        P("section", "expert", None),
        P("section", None, "expert"),
        P("section", None, "expert"),
    )
    out_specs = (
        P("section", "expert", None),
        P("section", "expert", None),
        P("section", "expert", None),
    )
    return jax.shard_map(body, mesh=mesh, in_specs=in_specs, out_specs=out_specs, check_vma=False)
```

```python
import functools
import math

import jax
import jax.numpy as jnp
import numpy as np
from jax import lax
from jax.experimental import pallas as pl
from jax.experimental.pallas import tpu as pltpu
from jax.sharding import PartitionSpec as P

FF = 2048
QUAD = 4
MESH = pl.DeviceIdType.MESH


def from_behind(value, axis, steps):
    count = lax.axis_size(axis)
    pairs = [(source, (source + steps) % count) for source in range(count)]
    return lax.ppermute(value, axis, pairs)


def routing(ids, gates, experts, capacity):
    expert_ids = jnp.arange(experts, dtype=jnp.int32)
    matches = ids[None, :, :] == expert_ids[:, None, None]
    routed = jnp.any(matches, axis=2)
    weights = jnp.sum(jnp.where(matches, gates[None, :, :], 0.0), axis=2)
    tokens = ids.shape[0]
    earlier = jnp.arange(tokens)[:, None] <= jnp.arange(tokens)[None, :]
    counted = jnp.sum(jnp.where(routed[:, :, None] & earlier[None], 1, 0), axis=1)
    position = counted - 1
    slot_ids = jnp.arange(capacity, dtype=jnp.int32)
    placing = (position[:, None, :] == slot_ids[None, :, None]) & routed[:, None, :]
    return (matches, placing.astype(jnp.float32), weights)


def xor(value, mask):
    out = value
    bit = 1
    while bit <= mask:
        if mask & bit:
            out = out + bit - 2 * bit * ((value // bit) % 2)
        bit *= 2
    return out


def dot(a, b, dims=((1,), (0,)), precision=None):
    return lax.dot_general(
        a, b, (dims, ((), ())), preferred_element_type=jnp.float32, precision=precision
    )


class Links:
    def __init__(self, send_sems, recv_sems):
        self.send_sems = send_sems
        self.recv_sems = recv_sems
        self.count = 0
        self.sent = []

    def copy(self, src, dst, peer, axis="expert"):
        k = self.count
        self.count += 1
        return pltpu.make_async_remote_copy(
            src_ref=src,
            dst_ref=dst,
            send_sem=self.send_sems.at[k],
            recv_sem=self.recv_sems.at[k],
            device_id={axis: peer},
            device_id_type=MESH,
        )

    def start(self, copy):
        copy.start()
        self.sent.append(copy)


def layer_kernel(
    slices,
    chunks,
    hop,
    tok_f,
    tok_b,
    w_gate,
    w_up,
    w_down,
    place_f,
    place_b,
    pre_gate,
    pre_up,
    rid_ref,
    fold_ref,
    unfold_ref,
    spread_ref,
    collect_ref,
    out_f,
    out_b,
    out_dots,
    tok,
    wc,
    wd,
    gat,
    par,
    rs1,
    rs2,
    rsz,
    hold,
    hold2,
    sums,
    landed,
    acc_ref,
    dot_ref,
    dot_got,
    local_sems,
    send_sems,
    recv_sems,
):
    device = lax.axis_index("expert")
    me = device % slices
    base = device - me
    lo = me % QUAD
    z = me // QUAD
    depth = slices // QUAD
    xp = base + xor(me, 1)
    yp = base + xor(me, 2)
    zp = [base + xor(z, q) * QUAD + lo for q in range(depth)]
    partners = [xp, yp] + zp[1:]
    width = wd.shape[2]
    ff = wd.shape[1]

    loads = []

    def load(src, dst):
        copy = pltpu.make_async_copy(src, dst, local_sems.at[len(loads)])
        loads.append(copy)
        copy.start()
        return copy

    load_tok = [load(tok_f, tok.at[0])]

    barrier = pltpu.get_barrier_semaphore()
    for peer in partners:
        pl.semaphore_signal(barrier, inc=1, device_id={"expert": peer}, device_id_type=MESH)
    greeted = len(partners)
    if hop:
        section = lax.axis_index("section")
        sections = lax.axis_size("section")
        ahead = (section + 1) % sections
        behind = (section + sections - 1) % sections
        for peer in (ahead, behind):
            pl.semaphore_signal(barrier, inc=1, device_id={"section": peer}, device_id_type=MESH)
        greeted += 2

    block_rows = gat.shape[2]
    group_rows = QUAD * block_rows
    places = (place_f, place_b)

    def place(mb):
        rid = rid_ref[:block_rows, :1]
        chosen = places[mb][...]
        total = jnp.zeros((block_rows, width), jnp.float32)
        for j in range(chunks):
            part = jnp.where(rid == j, chosen, 0.0).astype(jnp.bfloat16)
            total = total + dot(part, tok[mb, :, pl.ds(j * width, width)])
        gat[mb, me] = total.astype(jnp.bfloat16)

    links = Links(send_sems, recv_sems)

    def bid(q, mask):
        return xor(z, q) * QUAD + xor(lo, mask)

    order = list(range(1, depth)) + [0]
    steps = [(0, q) for q in range(depth)] + [(1, q) for q in order]
    tiles = width // 128
    cut = tiles // 2 * 128
    zsend, parts = {}, {}
    own_x, own_y, forward = {}, {}, {}
    r1, r2, rz = {}, {}, {}
    for step in steps:
        mb, q = step
        if step == steps[-1]:
            parts[step] = [(True, pl.ds(0, cut)), (False, pl.ds(cut, width - cut))]
        else:
            parts[step] = [(q % 2 == 0, pl.ds(0, width))]
        if q > 0:
            zsend[step] = links.copy(gat.at[mb, me], gat.at[mb, me], zp[q])
            rz[step] = links.copy(hold2.at[mb, q], rsz.at[mb, q], zp[q])
        own_x[step], own_y[step], forward[step], r1[step], r2[step] = [], [], [], [], []
        for first, cols in parts[step]:
            block = gat.at[mb, bid(q, 0), :, cols]
            own_x[step].append(links.copy(block, block, xp))
            own_y[step].append(links.copy(block, block, yp))
            got = gat.at[mb, bid(q, 2 if first else 1), :, cols]
            forward[step].append(links.copy(got, got, xp if first else yp))
            m1, p1, p2 = (1, xp, yp) if first else (2, yp, xp)
            r1[step].append([
                links.copy(par.at[mb, bid(q, 3), :, cols], rs1.at[mb, q, 1, :, cols], p1),
                links.copy(par.at[mb, bid(q, m1), :, cols], rs1.at[mb, q, 0, :, cols], p1),
            ])
            r2[step].append(links.copy(hold.at[mb, q, :, cols], rs2.at[mb, q, :, cols], p2))
    if hop:
        across = [
            links.copy(sums.at[0], landed.at[0], ahead, "section"),
            links.copy(sums.at[1], landed.at[1], behind, "section"),
        ]
    dx = links.copy(dot_ref.at[0], dot_got.at[0], xp)
    dy = links.copy(dot_ref.at[1], dot_got.at[1], yp)
    dz = [links.copy(dot_ref.at[2], dot_got.at[1 + q], zp[q]) for q in range(1, depth)]

    def own_sends(step):
        if step[1] > 0:
            zsend[step].wait_recv()
        for copy_x, copy_y in zip(own_x[step], own_y[step]):
            links.start(copy_x)
            links.start(copy_y)

    def start_mb(mb):
        for q in range(1, depth):
            links.start(zsend[mb, q])

    def do_forward(step):
        for k, (first, cols) in enumerate(parts[step]):
            (own_y if first else own_x)[step][k].wait_recv()
            links.start(forward[step][k])

    def compute(step):
        mb, q = step
        for k, (first, cols) in enumerate(parts[step]):
            (own_x if first else own_y)[step][k].wait_recv()
            forward[step][k].wait_recv()
        zq = xor(z, q)
        rid = rid_ref[...]
        group = pl.ds(zq * QUAD, QUAD)
        buf = gat[mb, group].reshape(group_rows, width)
        half = rid[:, :ff]
        fold = fold_ref[...]
        unfold = unfold_ref[...]
        if mb == 0:

            def gather_step(j, acc):
                return jnp.where(rid == j.astype(jnp.float32), dot(buf, wc[j]), acc)

            acc = lax.fori_loop(0, chunks, gather_step, jnp.zeros((group_rows, 2 * ff), jnp.float32))
            act = dot(fold, acc, precision=lax.Precision.HIGHEST)
            gate = act[:, :ff]
            hidden = gate / (1.0 + jnp.exp(-gate)) * act[:, ff:]
            spread = dot(unfold, hidden.astype(jnp.bfloat16))

            def piece(j, cols):
                part = jnp.where(half == j.astype(jnp.float32), spread, 0.0).astype(jnp.bfloat16)
                return dot(part, wd[j, :, cols])

        else:

            def gather_step(j, acc):
                return jnp.where(
                    half == j.astype(jnp.float32), dot(buf, wd[j], ((1,), (1,))), acc
                )

            acc = lax.fori_loop(0, chunks, gather_step, jnp.zeros((group_rows, ff), jnp.float32))
            grad = dot(fold, acc, precision=lax.Precision.HIGHEST)
            count = grad.shape[0]
            gate = pre_gate[zq].astype(jnp.float32)
            up = pre_up[zq].astype(jnp.float32)
            sig = 1.0 / (1.0 + jnp.exp(-gate))
            activated = gate * sig
            dots = jnp.sum(grad * activated * up, axis=1, keepdims=True)
            tile = dot(
                collect_ref[...], dots * spread_ref[...], precision=lax.Precision.HIGHEST
            )
            dot_ref[0, zq] = tile
            grad_gate = (grad * up * sig * (1.0 + gate * (1.0 - sig))).astype(jnp.bfloat16)
            grad_up = (grad * activated).astype(jnp.bfloat16)
            spread = jnp.concatenate([dot(unfold, grad_gate), dot(unfold, grad_up)], axis=1)

            def piece(j, cols):
                part = jnp.where(rid == j.astype(jnp.float32), spread, 0.0).astype(jnp.bfloat16)
                return dot(part, wc[j, cols, :], ((1,), (1,)))

        for k, (first, cols) in enumerate(parts[step]):
            acc_ref[:, cols] = piece(jnp.int32(0), cols)

            def out_step(j, carry):
                acc_ref[:, cols] += piece(j, cols)
                return carry

            lax.fori_loop(1, chunks, out_step, 0)
            done = acc_ref[:, cols].astype(jnp.bfloat16)
            par[mb, group, :, cols] = done.reshape(QUAD, block_rows, cols.size)
            for copy in r1[step][k]:
                links.start(copy)

    def wide(value):
        return value.astype(jnp.float32)

    def second(step):
        mb, q = step
        for k, (first, cols) in enumerate(parts[step]):
            r1[step][k][0].wait_recv()
            m2 = 2 if first else 1
            total = wide(par[mb, bid(q, m2), :, cols]) + wide(rs1[mb, q, 1, :, cols])
            hold[mb, q, :, cols] = total.astype(jnp.bfloat16)
            links.start(r2[step][k])

    def third(step):
        mb, q = step
        for k, (first, cols) in enumerate(parts[step]):
            r1[step][k][1].wait_recv()
            r2[step][k].wait_recv()
            total = wide(par[mb, bid(q, 0), :, cols]) + wide(rs1[mb, q, 0, :, cols])
            total = total + wide(rs2[mb, q, :, cols])
            hold2[mb, q, :, cols] = total.astype(jnp.bfloat16)
        if q > 0:
            links.start(rz[step])

    def finish(mb):
        total = wide(hold2[mb, 0])
        for q in range(1, depth):
            rz[mb, q].wait_recv()
            total = total + wide(rsz[mb, q])
        sums[mb] = total.astype(jnp.bfloat16)
        if hop:
            links.start(across[mb])

    def deliver(mb, out):
        if hop:
            across[mb].wait_recv()
            out[...] = landed[mb]
        else:
            out[...] = sums[mb]

    load_tok[0].wait()
    load_tok.append(load(tok_b, tok.at[1]))
    load_w = []
    for j in range(chunks):
        rows = pl.ds(j * width, width)
        load_w.append(load(w_gate.at[rows, :], wc.at[j, :, pl.ds(0, ff)]))
        load_w.append(load(w_up.at[rows, :], wc.at[j, :, pl.ds(ff, ff)]))
        load_w.append(load(w_down.at[:, rows], wd.at[j]))
    place(0)
    pl.semaphore_wait(barrier, greeted)
    own_sends(steps[0])
    start_mb(0)
    load_tok[1].wait()
    place(1)
    start_mb(1)
    count = len(steps)
    for t in range(count + 3):
        if t + 1 < count:
            own_sends(steps[t + 1])
        if t < count:
            do_forward(steps[t])
        if t == 0:
            for copy in load_w:
                copy.wait()
        if 0 <= t - 1 < count:
            compute(steps[t - 1])
        if t - 1 == count - 1:
            links.start(dx)
        if 0 <= t - 2 < count:
            second(steps[t - 2])
        if t - 2 == count - 1:
            dx.wait_recv()
            dot_ref[1] = dot_ref[0] + dot_got[0]
            links.start(dy)
        if 0 <= t - 3 < count:
            third(steps[t - 3])
        if t == count:
            finish(0)
        if t == count + 1:
            deliver(0, out_f)
    dy.wait_recv()
    dot_ref[2] = dot_ref[1] + dot_got[1]
    for copy in dz:
        links.start(copy)
    finish(1)
    total = dot_ref[2]
    for q in range(1, depth):
        dz[q - 1].wait_recv()
        total = total + dot_got[1 + q]
    out_dots[...] = total
    deliver(1, out_b)
    for copy in links.sent:
        copy.wait_send()


def run_layer(tok_f, tok_b, w_gate, w_up, w_down, place_f, place_b, pre_gate, pre_up, slices, rows, hop):
    features = tok_f.shape[1]
    chunks = 16 // math.gcd(16, rows)
    width = features // chunks
    ff = w_gate.shape[1]
    depth = slices // QUAD
    block_rows = chunks * rows
    group_rows = QUAD * block_rows
    group_slots = QUAD * rows

    row = np.arange(group_rows)
    slot = (row // block_rows) * rows + row % rows
    rid = np.broadcast_to((row % block_rows // rows)[:, None], (group_rows, 2 * ff))
    rid = rid.astype(np.float32)
    unfold = slot[:, None] == np.arange(group_slots)[None, :]
    fold = unfold.T.astype(np.float32)
    unfold = unfold.astype(jnp.bfloat16)
    slots = np.arange(group_slots)
    spread = (slots[:, None] % rows == np.arange(128)[None, :]).astype(np.float32)
    collect = (slots[None, :] // rows == np.arange(8)[:, None]).astype(np.float32)

    vmem = pl.BlockSpec(memory_space=pltpu.VMEM)
    anywhere = pl.BlockSpec(memory_space=pl.ANY)
    block = (block_rows, width)
    sems = 2 * (depth * 6 + 2 * (depth - 1)) + 6 + 2 + depth - 1 + 2
    return pl.pallas_call(
        functools.partial(layer_kernel, slices, chunks, hop),
        out_shape=(
            jax.ShapeDtypeStruct(block, jnp.bfloat16),
            jax.ShapeDtypeStruct(block, jnp.bfloat16),
            jax.ShapeDtypeStruct((depth, 8, 128), jnp.float32),
        ),
        in_specs=[anywhere] * 5 + [vmem] * 9,
        out_specs=(vmem, vmem, vmem),
        scratch_shapes=[
            pltpu.VMEM((2,) + tok_f.shape, jnp.bfloat16),
            pltpu.VMEM((chunks, width, 2 * ff), jnp.bfloat16),
            pltpu.VMEM((chunks, ff, width), jnp.bfloat16),
            pltpu.VMEM((2, slices) + block, jnp.bfloat16),
            pltpu.VMEM((2, slices) + block, jnp.bfloat16),
            pltpu.VMEM((2, depth, 2) + block, jnp.bfloat16),
            pltpu.VMEM((2, depth) + block, jnp.bfloat16),
            pltpu.VMEM((2, depth) + block, jnp.bfloat16),
            pltpu.VMEM((2, depth) + block, jnp.bfloat16),
            pltpu.VMEM((2, depth) + block, jnp.bfloat16),
            pltpu.VMEM((2,) + block, jnp.bfloat16),
            pltpu.VMEM((2,) + block, jnp.bfloat16),
            pltpu.VMEM((group_rows, width), jnp.float32),
            pltpu.VMEM((3, depth, 8, 128), jnp.float32),
            pltpu.VMEM((1 + depth, depth, 8, 128), jnp.float32),
            pltpu.SemaphoreType.DMA((2 + 3 * chunks,)),
            pltpu.SemaphoreType.DMA((sems,)),
            pltpu.SemaphoreType.DMA((sems,)),
        ],
        compiler_params=pltpu.CompilerParams(
            collective_id=0, has_side_effects=True, vmem_limit_bytes=56 * 2**20
        ),
        name="moe_layer",
    )(tok_f, tok_b, w_gate, w_up, w_down, place_f, place_b, pre_gate, pre_up,
      rid, fold, unfold, spread, collect)


def mix_kernel(rows, block_f, block_b, weight_f, weight_b, out_f, out_b):
    block_rows, width = block_f.shape
    j = pl.program_id(0)
    low = j * rows
    column = lax.broadcasted_iota(jnp.int32, weight_f.shape, 1)
    inside = (column >= low) & (column < low + rows)
    for block, weight, out in ((block_f, weight_f, out_f), (block_b, weight_b, out_b)):
        wanted = jnp.where(inside, weight[...], 0.0)
        high = wanted.astype(jnp.bfloat16)
        rest = (wanted - high.astype(jnp.float32)).astype(jnp.bfloat16)
        total = dot(jnp.concatenate([high, rest], axis=0), block[...])
        out[...] = (total[: high.shape[0]] + total[high.shape[0] :]).astype(jnp.bfloat16)


def mix(block_f, block_b, weight_f, weight_b, rows):
    block_rows, width = block_f.shape
    tokens = weight_f.shape[0]
    chunks = block_rows // rows
    whole = pl.BlockSpec(block_f.shape, lambda j: (0, 0))
    weights = pl.BlockSpec(weight_f.shape, lambda j: (0, 0))
    piece = pl.BlockSpec((tokens, width), lambda j: (0, j))
    shape = jax.ShapeDtypeStruct((tokens, chunks * width), jnp.bfloat16)
    return pl.pallas_call(
        functools.partial(mix_kernel, rows),
        out_shape=(shape, shape),
        grid=(chunks,),
        in_specs=[whole, whole, weights, weights],
        out_specs=(piece, piece),
        name="mix",
    )(block_f, block_b, weight_f, weight_b)


def body(
    act_in,
    cotangent,
    fwd_ids,
    fwd_gates,
    bwd_ids,
    bwd_gates,
    gate_w,
    up_w,
    down_w,
    gate_pre,
    up_pre,
):
    ndev = lax.axis_size("expert")
    ff_dev = gate_w.shape[2]
    slices = FF // ff_dev
    experts = ndev // slices
    capacity = gate_pre.shape[1] // ndev
    rows = experts * capacity
    chunks = 16 // math.gcd(16, rows)
    features = act_in.shape[2]
    width = features // chunks
    depth = slices // QUAD
    columns = [[g * slices + i for g in range(experts)] for i in range(slices)]

    def exchange(value):
        return lax.all_to_all(
            value, "expert", split_axis=0, concat_axis=0, axis_index_groups=columns, tiled=True
        )

    matches_f, placing_f, weights_f = routing(fwd_ids[0], fwd_gates[0], experts, capacity)
    matches_b, placing_b, weights_b = routing(bwd_ids[0], bwd_gates[0], experts, capacity)

    def prepare(tokens, placing):
        chosen = placing.reshape(rows, tokens.shape[0])
        if experts > 1:
            picked = dot(chosen.astype(jnp.bfloat16), tokens).astype(jnp.bfloat16)
            picked = exchange(picked.reshape(experts, capacity, features))
            tokens = picked.reshape(rows, features)
            chosen = jnp.eye(rows, dtype=jnp.float32)
        return tokens, jnp.tile(chosen, (chunks, 1))

    tok_f, place_f = prepare(act_in[0], placing_f)
    tok_b, place_b = prepare(cotangent[0], placing_b)

    def by_group(saved):
        saved = saved.reshape(experts, slices, capacity, ff_dev).transpose(1, 0, 2, 3)
        return saved.reshape(depth, QUAD * rows, ff_dev)

    block_f, block_b, dots = run_layer(
        tok_f, tok_b, gate_w[0], up_w[0], down_w[0], place_f, place_b,
        by_group(gate_pre[0]), by_group(up_pre[0]), slices, rows, experts == 1,
    )
    me = lax.axis_index("expert") % slices
    mine = lax.dynamic_slice(dots, (me // QUAD, me % QUAD, 0), (1, 1, 128))
    mine = mine[0, 0, :rows].reshape(experts, capacity)

    def send_back(block):
        table = block.reshape(chunks, rows, width).transpose(1, 0, 2)
        table = exchange(table.reshape(experts, capacity, features))
        table = table.reshape(rows, chunks, width).transpose(1, 0, 2)
        return table.reshape(chunks * rows, width)

    if experts > 1:
        block_f = send_back(block_f)
        block_b = send_back(block_b)
        mine = exchange(mine)

    token_dots = jnp.sum(placing_b * mine[:, :, None], axis=1)
    gate_grad = jnp.sum(jnp.where(matches_b, token_dots[:, :, None], 0.0), axis=0)

    def weight_table(placing, weights):
        table = (placing * weights[:, None, :]).reshape(rows, -1).T
        return jnp.tile(table, (1, chunks))

    weight_f = from_behind(weight_table(placing_f, weights_f), "section", 1)
    weight_b = from_behind(weight_table(placing_b, weights_b), "section", -1)
    if experts > 1:
        block_f = from_behind(block_f, "section", 1)
        block_b = from_behind(block_b, "section", -1)
    next_act, prev_grad = mix(block_f, block_b, weight_f, weight_b, rows)
    return (next_act[None], prev_grad[None], gate_grad[None])


def solution(mesh):
    in_specs = (
        P("section", "expert", None),
        P("section", "expert", None),
        P("section", "expert", None),
        P("section", "expert", None),
        P("section", "expert", None),
        P("section", "expert", None),
        P("section", None, "expert"),
        P("section", None, "expert"),
        P("section", "expert", None),
        P("section", None, "expert"),
        P("section", None, "expert"),
    )
    out_specs = (
        P("section", "expert", None),
        P("section", "expert", None),
        P("section", "expert", None),
    )
    return jax.shard_map(body, mesh=mesh, in_specs=in_specs, out_specs=out_specs, check_vma=False)
```
